32 devices in a mesh: tok: 4 (over z), hid: 8 (over y, x, core).
Axes of the slice: x: 2, y: 2, z: 4, core: 2. Of those that a mesh axis runs over, the one named last changes fastest.
Arguments:
- activations: bfloat16 [512, 4096], P('tok'), may hold values from -12 to 12
- cotangent: bfloat16 [512, 8192], P('tok', 'hid'), may hold values from -0.015625 to 0.015625
- left_gram: float32 [32, 1024, 1024], P('hid', 'tok'), may hold values from -0.28125 to 30, as said below
- right_gram: float32 [32, 1024, 1024], P('hid', 'tok'), may hold values from -0.28125 to 30, as said below
- left_root: float32 [32, 1024, 1024], P('hid', 'tok'), may hold values from -0.0115625 to 1.21, as said below
- right_root: float32 [32, 1024, 1024], P('hid', 'tok'), may hold values from -0.0115625 to 1.21, as said below
Outputs:
- left_next: float32 [32, 1024, 1024], P('hid', 'tok')
- right_next: float32 [32, 1024, 1024], P('hid', 'tok')
- left_refined: float32 [32, 1024, 1024], P('hid', 'tok')
- right_refined: float32 [32, 1024, 1024], P('hid', 'tok')
- update: float32 [4, 1024, 8192], P(None, 'tok', 'hid')
The draws below stay inside these ranges and needn't reach their ends.
Inputs may be any that keep to these rules, and one draw needn't show every extreme that they name: `left_gram`: every block is symmetric and positive definite. `right_gram`: every block is symmetric and positive definite. `left_root`: every block is symmetric. `right_root`: every block is symmetric.
All inputs are finite; a program needn't handle non-finite values.
Results may differ from the reference program's by a relative error of at most 0.019.
Values may be sent and summed in bfloat16 or wider, within the bound.
A program may use at most 128 MiB of HBM per device.

```python
import jax
import jax.numpy as jnp
from jax import lax

DW = 4096
FF = 8192
BS = 1024
TOKENS = 512
NBR = 4
NBC = 8
NB = 32
N_TOK = 4


def draw_activations(key, part):
    noise_key = jax.random.fold_in(key, 1)
    scale_key = jax.random.fold_in(key, 2)
    values = jnp.clip(jax.random.normal(noise_key, (TOKENS, DW), jnp.float32), -6.0, 6.0)
    rising = (jnp.arange(DW) % BS).astype(jnp.float32) / BS
    spread = jax.random.uniform(scale_key, (DW,), jnp.float32)
    scales = jnp.exp(jnp.log(2.0) * 0.5 * (spread + rising))
    return (values * scales[None, :]).astype(jnp.bfloat16)


def scales_from(unit):
    upper = 10.0
    return jnp.exp(unit * jnp.log(upper))


def coupling_from(raw):
    raw = 0.5 * (raw + jnp.swapaxes(raw, 1, 2))
    identity = jnp.eye(BS, dtype=jnp.float32)
    return raw * (1.0 - identity) * (0.3 / BS ** 0.5) + identity


def gram_from(unit, raw):
    scales = jnp.sqrt(scales_from(unit))
    return scales[:, :, None] * coupling_from(raw) * scales[:, None, :]


def root_from(unit, jitter, raw):
    factors = jitter * scales_from(unit) ** (-0.25)
    return factors[:, :, None] * coupling_from(raw) * factors[:, None, :]


def draw_left_gram(key, part):
    unit = jax.random.uniform(jax.random.fold_in(key, 11), (NB, BS), jnp.float32)
    raw = jax.random.uniform(jax.random.fold_in(key, 12), (NB, BS, BS), jnp.float32, -1.0, 1.0)
    return gram_from(unit, raw)


def draw_right_gram(key, part):
    unit = jax.random.uniform(jax.random.fold_in(key, 21), (NB, BS), jnp.float32)
    raw = jax.random.uniform(jax.random.fold_in(key, 22), (NB, BS, BS), jnp.float32, -1.0, 1.0)
    return gram_from(unit, raw)


def draw_left_root(key, part):
    unit = jax.random.uniform(jax.random.fold_in(key, 11), (NB, BS), jnp.float32)
    jitter = jax.random.uniform(jax.random.fold_in(key, 13), (NB, BS), jnp.float32, 0.9, 1.1)
    raw = jax.random.uniform(jax.random.fold_in(key, 14), (NB, BS, BS), jnp.float32, -1.0, 1.0)
    return root_from(unit, jitter, raw)


def draw_right_root(key, part):
    unit = jax.random.uniform(jax.random.fold_in(key, 21), (NB, BS), jnp.float32)
    jitter = jax.random.uniform(jax.random.fold_in(key, 23), (NB, BS), jnp.float32, 0.9, 1.1)
    raw = jax.random.uniform(jax.random.fold_in(key, 24), (NB, BS, BS), jnp.float32, -1.0, 1.0)
    return root_from(unit, jitter, raw)


def block_levels(own_key, shape, cuts, least, largest):
    def one(axis_at, blocks):
        heights = jax.random.uniform(jax.random.fold_in(jax.random.fold_in(own_key, 6), axis_at), (blocks,), jnp.float32, least / len(cuts), largest / len(cuts))
        return jnp.repeat(jnp.exp(heights), shape[axis_at] // blocks).reshape((-1,) + (1,) * (len(shape) - axis_at - 1))

    level = one(*cuts[0])
    for cut in cuts[1:]:
        level = level * one(*cut)
    return level


def bell_draw(own_key, shape, deviation, reach, cuts=(), kind=jnp.bfloat16):
    gain = block_levels(own_key, shape, cuts, -0.22, 0.18) if cuts else 1.0
    array = jax.random.normal(own_key, shape, jnp.float32) * deviation * gain
    return jnp.minimum(jnp.maximum(array, -reach), reach).astype(kind)


def setup_inputs(seed: int = 0) -> dict:
    key_list = jax.random.split(jax.random.key(seed), 7)
    activations = draw_activations(jax.random.fold_in(key_list[6], 71), 0)
    cotangent = bell_draw(key_list[1], (TOKENS, FF), (0.0221 / TOKENS ** 0.5), 0.015625, ((0, 4), (1, 8)))
    left_gram = draw_left_gram(jax.random.fold_in(key_list[6], 71), 0)
    right_gram = draw_right_gram(jax.random.fold_in(key_list[6], 71), 0)
    left_root = draw_left_root(jax.random.fold_in(key_list[6], 71), 0)
    right_root = draw_right_root(jax.random.fold_in(key_list[6], 71), 0)
    return {"activations": activations, "cotangent": cotangent, "left_gram": left_gram, "right_gram": right_gram, "left_root": left_root, "right_root": right_root}


BETA = 0.95
EPS = 1e-06

def newton_root(gram_block, root_block, root_low):
    product = gram_block.astype(jnp.bfloat16)
    for repeat in range(4):
        product = jnp.dot(product, root_low, preferred_element_type=jnp.float32).astype(jnp.bfloat16)
    final = jnp.dot(product, root_low, preferred_element_type=jnp.float32)
    return (5.0 * root_block - final) / 4.0

def reference(activations, cotangent, left_gram, right_gram, left_root, right_root):
    shard_inputs = activations.reshape(N_TOK, TOKENS // N_TOK, DW)
    shard_cotangents = cotangent.reshape(N_TOK, TOKENS // N_TOK, FF)

    def accumulate(running, shards):
        partial_value = jnp.dot(shards[0].T, shards[1], preferred_element_type=jnp.float32)
        rounded = lax.optimization_barrier(partial_value.astype(jnp.bfloat16))
        return (running + rounded.astype(jnp.float32), None)
    gradient, unused = lax.scan(accumulate, jnp.zeros((DW, FF), jnp.float32), (shard_inputs, shard_cotangents))
    grad_low = gradient.astype(jnp.bfloat16)
    blocks = grad_low.reshape(NBR, BS, NBC, BS).transpose(2, 0, 1, 3).reshape(NB, BS, BS)

    def per_block(members):
        grad_block, left_old, right_old, left_current, right_current = members
        left_low = left_current.astype(jnp.bfloat16)
        right_low = right_current.astype(jnp.bfloat16)
        left_new = BETA * left_old + jnp.dot(grad_block, grad_block.T, preferred_element_type=jnp.float32)
        right_new = BETA * right_old + jnp.dot(grad_block.T, grad_block, preferred_element_type=jnp.float32)
        inner = jnp.dot(left_low, grad_block, preferred_element_type=jnp.float32).astype(jnp.bfloat16)
        precond = jnp.dot(inner, right_low, preferred_element_type=jnp.float32)
        scale = jnp.sqrt(jnp.sum(precond * precond) / (BS * BS) + EPS)
        return (left_new, right_new, newton_root(left_new, left_current, left_low), newton_root(right_new, right_current, right_low), precond / scale)
    results = lax.map(per_block, (blocks, left_gram, right_gram, left_root, right_root))
    update = results[4].reshape(NBC, NBR, BS, BS).transpose(1, 2, 0, 3).reshape(NBR, BS, FF)
    return (results[0], results[1], results[2], results[3], update)
```

```python
import functools

import jax
import jax.numpy as jnp
from jax import lax
from jax.experimental import pallas as pl
from jax.experimental.pallas import tpu as pltpu
from jax.sharding import PartitionSpec as P


BETA = 0.95
EPS = 1e-06


def as_sent(value):

    def short(part):
        return part.astype(jnp.bfloat16) if part.dtype == jnp.float32 else part

    return jax.tree.map(short, value)


def partner(block, axis, bit):
    count = lax.axis_size(axis)
    route = []
    for low in range(count):
        high = low | 1 << bit
        if high != low and high < count:
            route += [(low, high), (high, low)]
    return lax.ppermute(block, axis, route)


def newton_rows(gram_rows, root_full, root_rows):
    product = gram_rows.astype(jnp.bfloat16)
    for _ in range(4):
        product = jnp.einsum(
            "brk,bkc->brc", product, root_full, preferred_element_type=jnp.float32
        ).astype(jnp.bfloat16)
    final = jnp.einsum("brk,bkc->brc", product, root_full, preferred_element_type=jnp.float32)
    return (5.0 * root_rows - final) / 4.0


def butterfly(pieces, swapper):
    group_size = pieces.shape[0]
    position = lax.axis_index("hid") % group_size
    ordering = jnp.bitwise_xor(jnp.arange(group_size, dtype=jnp.int32), position)
    holding = jnp.take(pieces, ordering, axis=0)
    for bit_level in range(group_size.bit_length() - 1):
        stride = 1 << bit_level
        shaped = holding.reshape((group_size // (2 * stride), 2, stride) + holding.shape[1:])
        incoming = swapper(shaped[:, 1], bit_level)
        holding = jnp.stack([shaped[:, 0], incoming], axis=1).reshape(holding.shape)
    return jnp.take(holding, ordering, axis=0)


def swap_blocks(portion, bit_level):
    return jax.tree.map(
        lambda part, own: part.astype(own.dtype),
        partner(as_sent(portion), "hid", bit_level),
        portion,
    )


def swap_updates(portion, bit_level):
    return jax.tree.map(
        lambda part, own: part.astype(own.dtype),
        partner(as_sent(portion), "hid", bit_level),
        portion,
    )


def make_folder(own_rows, root_low_rows, first_row):
    slab_rows = own_rows.shape[1]

    def absorb(running, portion, offset):
        column_slab = lax.dynamic_slice_in_dim(portion, first_row, slab_rows, 2)
        products = jnp.einsum("brk,bnk->brn", own_rows, portion, preferred_element_type=jnp.float32)
        right_rows = jnp.einsum(
            "bnr,bnk->brk", column_slab, portion, preferred_element_type=jnp.float32
        )
        left_applied = jnp.einsum(
            "brn,bnk->brk", root_low_rows, portion, preferred_element_type=jnp.float32
        )
        return (products, right_rows, left_applied)

    return absorb


def on_device(activations, cotangent, left_gram, right_gram, left_root, right_root):
    owned_blocks, slab_rows, block_size = left_gram.shape
    slab_width = cotangent.shape[1]
    group_size = block_size // slab_width
    block_rows = activations.shape[1] // block_size
    partial_value = jnp.einsum(
        "td,tc->dc", activations, cotangent, preferred_element_type=jnp.float32
    )
    partial_value = partial_value.reshape(block_rows, block_size, slab_width)
    first_row = lax.axis_index("tok") * slab_rows
    left_low = left_root.astype(jnp.bfloat16)
    right_low = right_root.astype(jnp.bfloat16)
    left_full, right_full = (
        lax.all_gather(left_low, "tok", axis=1, tiled=True),
        lax.all_gather(right_low, "tok", axis=1, tiled=True),
    )
    empty = jnp.zeros((owned_blocks, slab_rows, block_size), jnp.float32)
    initial = (empty, empty, empty)
    summed = lax.psum(partial_value.astype(jnp.bfloat16), "tok")
    pieces = summed.reshape(group_size, owned_blocks, block_size, slab_width)
    arrived = butterfly(pieces, swap_blocks)
    full_block = arrived.transpose(1, 2, 0, 3).reshape(owned_blocks, block_size, block_size)
    own_rows = lax.dynamic_slice_in_dim(full_block, first_row, slab_rows, 1)
    folder = make_folder(own_rows, left_low, first_row)
    left_cols, right_rows, left_applied = folder(initial, full_block, 0)
    left_next = BETA * left_gram + left_cols
    right_next = BETA * right_gram + right_rows
    left_refined = newton_rows(left_next, left_full, left_root)
    right_refined = newton_rows(right_next, right_full, right_root)
    precond = jnp.einsum(
        "brk,bkc->brc",
        left_applied.astype(jnp.bfloat16),
        right_full,
        preferred_element_type=jnp.float32,
    )
    squares = lax.psum(jnp.sum(precond * precond, axis=(1, 2)), "tok")
    scale = jnp.sqrt(squares / (block_size * block_size) + EPS)
    scaled = precond / scale[:, None, None]
    outgoing = scaled.reshape(owned_blocks, slab_rows, group_size, slab_width).transpose(2, 0, 1, 3)
    returned = butterfly(outgoing, swap_updates)
    update = returned.reshape(block_rows, slab_rows, slab_width)
    return (left_next, right_next, left_refined, right_refined, update)


RIGHT_PARTS = (4,)
LEFT_PARTS = (2, 2)
VMEM = 60 * 1024 * 1024


def part_ranges(sizes, blocks):
    if sum(sizes) != blocks:
        sizes = (blocks,)
    ranges, first = [], 0
    for size in sizes:
        ranges.append((first, size))
        first += size
    return ranges


def pair_swap(value, axis, mask):
    count = lax.axis_size(axis)
    return lax.ppermute(value, axis, [(i, i ^ mask) for i in range(count)])


def strip_rows(blocks):
    return -(-blocks // 16) * 16


def diagonal_masks(half):
    row = lax.broadcasted_iota(jnp.int32, (half, half), 0)
    column = lax.broadcasted_iota(jnp.int32, (half, half), 1)
    return row, column


def pack_body(ranges, root_ref, fold_ref, *outs):
    total = ranges[-1][0] + ranges[-1][1]
    tile = root_ref.shape[1]
    half = tile // 2
    b = pl.program_id(0)
    me = lax.axis_index("tok")
    low = me < 2

    def tile_at(index):
        return root_ref[0, :, pl.ds(pl.multiple_of(index * tile, tile), tile)]

    own = tile_at(me)
    first, last = own[:half, :half], own[half:, half:]
    row, column = diagonal_masks(half)
    folded = jnp.where(row <= column, first, last)
    place = pl.ds(pl.multiple_of(b * half, half), half)
    fold_ref[place, :half] = folded.astype(jnp.bfloat16)
    fold_ref[place, half:] = own[:half, half:].astype(jnp.bfloat16)
    diagonal = jnp.sum(jnp.where(row == column, last, 0.0), axis=0, keepdims=True)
    strip = strip_rows(total)
    strip_at = pl.ds(total * half, strip)
    line = lax.broadcasted_iota(jnp.int32, (strip, half), 0)

    @pl.when(b == 0)
    def _():
        fold_ref[strip_at, :] = jnp.zeros((strip, tile), jnp.bfloat16)

    held = fold_ref[strip_at, :half].astype(jnp.float32)
    fold_ref[strip_at, :half] = jnp.where(line == b, diagonal, held).astype(jnp.bfloat16)
    near = jnp.where(low, 2, 1)
    far = jnp.where(low, 3, 0)
    mate = jnp.where(me % 2 == 0, me + 1, me - 1)
    for at, (start, size) in enumerate(ranges):
        wide, thin = outs[2 * at], outs[2 * at + 1]

        @pl.when((b >= start) & (b < start + size))
        def _():
            slot = b - start
            wide[pl.ds(pl.multiple_of(slot * 2 * tile, tile), tile), :] = tile_at(near).astype(jnp.bfloat16)
            wide[pl.ds(pl.multiple_of(slot * 2 * tile + tile, tile), tile), :] = tile_at(far).astype(jnp.bfloat16)
            thin[pl.ds(pl.multiple_of(slot * tile, tile), tile), :] = tile_at(mate).astype(jnp.bfloat16)


def pack(roots, ranges):
    blocks, tile, order = roots.shape
    shapes = [jax.ShapeDtypeStruct((blocks * (tile // 2) + strip_rows(blocks), tile), jnp.bfloat16)]
    for _, size in ranges:
        shapes.append(jax.ShapeDtypeStruct((size * 2 * tile, tile), jnp.bfloat16))
        shapes.append(jax.ShapeDtypeStruct((size * tile, tile), jnp.bfloat16))
    return pl.pallas_call(
        functools.partial(pack_body, ranges),
        grid=(blocks,),
        in_specs=[pl.BlockSpec((1, tile, order), lambda b: (b, 0, 0))],
        out_specs=[pl.BlockSpec(one.shape, lambda b: (0, 0)) for one in shapes],
        out_shape=shapes,
        cost_estimate=pl.CostEstimate(
            flops=2 * blocks * tile * order, bytes_accessed=6 * blocks * tile * order, transcendentals=0
        ),
        compiler_params=pltpu.CompilerParams(vmem_limit_bytes=VMEM),
    )(roots)


def exchange(roots, ranges):
    fold, *rest = pack(roots, ranges)
    folds = []
    for mask in (1, 2, 3):
        folds.append(pair_swap(fold, "tok", mask))
    parts = []
    for at in range(len(ranges)):
        wide, thin = rest[2 * at], rest[2 * at + 1]
        wide = pair_swap(wide, "tok", 1)
        skip = lax.ppermute(thin, "tok", [(2, 0), (1, 3)])
        following = lax.ppermute(thin, "tok", [(2, 1), (1, 2)])
        parts.append((wide, skip, following))
    return folds, parts


def front_body(place_ref, act, cot, left_gram, right_gram, left_root, pieces, left_next, right_next, applied, tokens, grad):
    b = pl.program_id(0)
    rows, order = left_gram.shape[1:]
    group, width = act.shape[0], pieces[0].shape[1]
    hid, first_row = place_ref[0], place_ref[1] * rows

    @pl.when(b == 0)
    def _():
        tokens[:group, :] = act[...]
        for mask, piece in enumerate(pieces):
            column = jnp.bitwise_xor(hid, mask) * width
            tokens[group:, pl.ds(pl.multiple_of(column, width), width)] = piece[...]

    both = (((0,), (0,)), ((), ()))

    @pl.loop(0, order // rows)
    def _(step):
        column = pl.multiple_of(b * order + step * rows, rows)
        grad[pl.ds(pl.multiple_of(step * rows, rows), rows), :] = lax.dot_general(
            tokens[:, pl.ds(column, rows)], cot[...], both, preferred_element_type=jnp.float32
        ).astype(jnp.bfloat16)

    slab = pl.ds(pl.multiple_of(first_row, rows), rows)
    product = lax.dot_general(
        grad[slab, :], grad[...], (((1,), (1,)), ((), ())), preferred_element_type=jnp.float32
    )
    left_next[0] = BETA * left_gram[0] + product
    product = lax.dot_general(grad[:, slab], grad[...], both, preferred_element_type=jnp.float32)
    right_next[0] = BETA * right_gram[0] + product
    applied[0] = jnp.dot(
        left_root[0].astype(jnp.bfloat16), grad[...], preferred_element_type=jnp.float32
    ).astype(jnp.bfloat16)


def front(place, act, cot, pieces, left_gram, right_gram, left_root):
    blocks, rows, order = left_gram.shape
    count = len(pieces)
    depth = cot.shape[0]

    def body(place_ref, act_ref, cot_ref, lg, rg, lr, *refs):
        front_body(place_ref, act_ref, cot_ref, lg, rg, lr, refs[:count], *refs[count:])

    def whole(array):
        return pl.BlockSpec(array.shape, lambda b, s: (0,) * array.ndim)

    slab = pl.BlockSpec((1, rows, order), lambda b, s: (b, 0, 0))
    shape = (blocks, rows, order)
    return pl.pallas_call(
        body,
        grid_spec=pltpu.PrefetchScalarGridSpec(
            num_scalar_prefetch=1,
            grid=(blocks,),
            in_specs=[whole(act), whole(cot), slab, slab, slab] + [whole(one) for one in pieces],
            out_specs=[slab, slab, slab],
            scratch_shapes=[
                pltpu.VMEM((depth, act.shape[1]), jnp.bfloat16),
                pltpu.VMEM((order, order), jnp.bfloat16),
            ],
        ),
        out_shape=[
            jax.ShapeDtypeStruct(shape, jnp.float32),
            jax.ShapeDtypeStruct(shape, jnp.float32),
            jax.ShapeDtypeStruct(shape, jnp.bfloat16),
        ],
        cost_estimate=pl.CostEstimate(
            flops=2 * blocks * order * order * (depth + 3 * rows),
            bytes_accessed=blocks * rows * order * 22,
            transcendentals=0,
        ),
        compiler_params=pltpu.CompilerParams(vmem_limit_bytes=VMEM),
    )(place, act, cot, left_gram, right_gram, left_root, *pieces)


def chain_body(first, total, with_update, with_base, *refs):
    next_ref, root_ref, fold1, fold2, fold3, wide, skip, following = refs[:8]
    refs = refs[8:]
    if with_update:
        applied, refs = refs[0], refs[1:]
    if with_base:
        refs = refs[1:]
    refined, refs = refs[0], refs[1:]
    if with_update:
        precond, refs = refs[0], refs[1:]
    full, product = refs
    tile = root_ref.shape[1]
    half = tile // 2
    slot = pl.program_id(0)
    b = slot + first
    me = lax.axis_index("tok")
    low = me < 2
    end = (me == 0) | (me == 3)
    near = jnp.where(low, 2, 1)
    far = jnp.where(low, 3, 0)
    mate = jnp.where(me % 2 == 0, me + 1, me - 1)

    def at(index, extra=0, size=tile):
        return pl.ds(pl.multiple_of(index * tile + extra, half), size)

    def flipped(value):
        return value.astype(jnp.float32).T.astype(jnp.bfloat16)

    full[at(me), :] = root_ref[0].astype(jnp.bfloat16)
    for other in (mate, near, far):
        full[at(other), at(me)] = root_ref[0, :, at(other)].T.astype(jnp.bfloat16)
    row, column = diagonal_masks(half)
    strip = strip_rows(total)
    line = lax.broadcasted_iota(jnp.int32, (strip, half), 0)
    place = pl.ds(pl.multiple_of(b * half, half), half)

    def unfold(index, fold):
        folded = fold[place, :half].astype(jnp.float32)
        corner = fold[place, half:]
        turned = folded.T
        strips = fold[pl.ds(total * half, strip), :half].astype(jnp.float32)
        diagonal = jnp.sum(jnp.where(line == b, strips, 0.0), axis=0, keepdims=True)
        full[at(index, 0, half), at(index, 0, half)] = jnp.where(row <= column, folded, turned).astype(jnp.bfloat16)
        lower = jnp.where(row == column, diagonal, jnp.where(row > column, folded, turned))
        full[at(index, half, half), at(index, half, half)] = lower.astype(jnp.bfloat16)
        full[at(index, 0, half), at(index, half, half)] = corner
        full[at(index, half, half), at(index, 0, half)] = flipped(corner)

    def both(i, j, value):
        full[at(i), at(j)] = value
        full[at(j), at(i)] = flipped(value)

    unfold(mate, fold1)
    unfold(jnp.where(low, me + 2, me - 2), fold2)
    unfold(3 - me, fold3)
    both(mate, near, wide[pl.ds(pl.multiple_of(slot * 2 * tile, tile), tile), :])
    both(mate, far, wide[pl.ds(pl.multiple_of(slot * 2 * tile + tile, tile), tile), :])
    thin = pl.ds(pl.multiple_of(slot * tile, tile), tile)
    both(near, far, jnp.where(end, skip[thin, :], following[thin, :]))
    if with_update:
        precond[0] = jnp.dot(applied[0], full[...], preferred_element_type=jnp.float32)
    product[...] = next_ref[0].astype(jnp.bfloat16)

    @pl.loop(0, 4)
    def _(repeat):
        product[...] = jnp.dot(
            product[...], full[...], preferred_element_type=jnp.float32
        ).astype(jnp.bfloat16)

    final = jnp.dot(product[...], full[...], preferred_element_type=jnp.float32)
    refined[0] = (5.0 * root_ref[0] - final) / 4.0


def chain(next_rows, roots, folds, tiles, applied, base, first, size):
    blocks, rows, order = roots.shape

    def slab(array):
        return pl.BlockSpec((1,) + array.shape[1:], lambda b: (b + first, 0, 0))

    def whole(array):
        return pl.BlockSpec(array.shape, lambda b: (0, 0))

    operands = [next_rows, roots, *folds, *tiles]
    specs = [slab(next_rows), slab(roots)] + [whole(one) for one in (*folds, *tiles)]
    if applied is not None:
        operands.append(applied)
        specs.append(slab(applied))
    aliases = {}
    if base is not None:
        aliases = {len(operands): 0}
        operands.append(base)
        specs.append(pl.BlockSpec(memory_space=pl.ANY))
    out = jax.ShapeDtypeStruct((blocks, rows, order), jnp.float32)
    outputs = [out] if applied is None else [out, out]
    matmuls = 5 if applied is None else 6
    return pl.pallas_call(
        functools.partial(chain_body, first, blocks, applied is not None, base is not None),
        grid=(size,),
        in_specs=specs,
        out_specs=[slab(one) for one in outputs],
        out_shape=outputs,
        input_output_aliases=aliases,
        scratch_shapes=[
            pltpu.VMEM((order, order), jnp.bfloat16),
            pltpu.VMEM((rows, order), jnp.bfloat16),
        ],
        cost_estimate=pl.CostEstimate(
            flops=2 * matmuls * size * rows * order * order,
            bytes_accessed=size * rows * order * 20,
            transcendentals=0,
        ),
        compiler_params=pltpu.CompilerParams(vmem_limit_bytes=VMEM),
    )(*operands)


def gather_tokens(activations, cotangent):
    count = lax.axis_size("hid")
    place = lax.axis_index("hid")
    width = activations.shape[1] // count
    piece = lax.dynamic_slice_in_dim(activations, place * width, width, 1)
    arrived, cots = [], [cotangent]
    for mask in (1, 2, 3):
        arrived.append(pair_swap(piece, "tok", mask))
    for mask in (1, 2, 3):
        cots.append(pair_swap(cotangent, "tok", mask))
    mine = jnp.concatenate(arrived, axis=0)
    held = [mine]
    for mask in range(2, count, 2):
        held.append(pair_swap(mine, "hid", mask))
    pieces = []
    for one in held:
        pieces += [one, pair_swap(one, "hid", 1)]
    return pieces, jnp.concatenate(cots, axis=0)


def line_program(activations, cotangent, left_gram, right_gram, left_root, right_root):
    blocks, _, order = left_gram.shape
    right_ranges = part_ranges(RIGHT_PARTS, blocks)
    left_ranges = part_ranges(LEFT_PARTS, blocks)
    pieces, cots = gather_tokens(activations, cotangent)
    right_folds, right_tiles = exchange(right_root, right_ranges)
    left_folds, left_tiles = exchange(left_root, left_ranges)
    place = jnp.stack([lax.axis_index("hid"), lax.axis_index("tok")]).astype(jnp.int32)
    left_next, right_next, applied = front(
        place, activations, cots, pieces, left_gram, right_gram, left_root
    )
    (first, size), = right_ranges
    right_refined, precond = chain(
        right_next, right_root, right_folds, right_tiles[0], applied, None, first, size
    )
    local = jnp.sum(precond * precond, axis=(1, 2))
    squares = local
    for mask in (1, 2, 3):
        squares = squares + pair_swap(local, "tok", mask)
    scale = jnp.sqrt(squares / (order * order) + EPS)
    update = precond / scale[:, None, None]
    left_refined = None
    for at, (first, size) in enumerate(left_ranges):
        (left_refined,) = chain(
            left_next, left_root, left_folds, left_tiles[at], None, left_refined, first, size
        )
    return left_next, right_next, left_refined, right_refined, update


def solution(mesh):
    in_specs = (
        P("tok", None),
        P("tok", "hid"),
        P("hid", "tok", None),
        P("hid", "tok", None),
        P("hid", "tok", None),
        P("hid", "tok", None),
    )
    out_specs = (
        P("hid", "tok", None),
        P("hid", "tok", None),
        P("hid", "tok", None),
        P("hid", "tok", None),
        P(None, "tok", "hid"),
    )

    def run(*operands):
        activations, cotangent, left_gram = (one.shape for one in operands[:3])
        tok, hid = mesh.shape["tok"], mesh.shape["hid"]
        whole_blocks = cotangent[1] == left_gram[2]
        one_column = left_gram[0] == activations[1] // left_gram[2]
        even = hid >= 2 and hid & (hid - 1) == 0
        if tok == 4 and whole_blocks and one_column and even:
            return line_program(*operands)
        return on_device(*operands)

    return jax.shard_map(
        run, mesh=mesh, in_specs=in_specs, out_specs=out_specs, check_vma=False
    )
```

```python
import functools

import jax
import jax.numpy as jnp
from jax import lax
from jax.experimental import pallas as pl
from jax.experimental.pallas import tpu as pltpu
from jax.sharding import PartitionSpec as P


BETA = 0.95
EPS = 1e-06


def as_sent(value):

    def short(part):
        return part.astype(jnp.bfloat16) if part.dtype == jnp.float32 else part

    return jax.tree.map(short, value)


def partner(block, axis, bit):
    count = lax.axis_size(axis)
    route = []
    for low in range(count):
        high = low | 1 << bit
        if high != low and high < count:
            route += [(low, high), (high, low)]
    return lax.ppermute(block, axis, route)


def newton_rows(gram_rows, root_full, root_rows):
    product = gram_rows.astype(jnp.bfloat16)
    for _ in range(4):
        product = jnp.einsum(
            "brk,bkc->brc", product, root_full, preferred_element_type=jnp.float32
        ).astype(jnp.bfloat16)
    final = jnp.einsum("brk,bkc->brc", product, root_full, preferred_element_type=jnp.float32)
    return (5.0 * root_rows - final) / 4.0


def butterfly(pieces, swapper):
    group_size = pieces.shape[0]
    position = lax.axis_index("hid") % group_size
    ordering = jnp.bitwise_xor(jnp.arange(group_size, dtype=jnp.int32), position)
    holding = jnp.take(pieces, ordering, axis=0)
    for bit_level in range(group_size.bit_length() - 1):
        stride = 1 << bit_level
        shaped = holding.reshape((group_size // (2 * stride), 2, stride) + holding.shape[1:])
        incoming = swapper(shaped[:, 1], bit_level)
        holding = jnp.stack([shaped[:, 0], incoming], axis=1).reshape(holding.shape)
    return jnp.take(holding, ordering, axis=0)


def swap_blocks(portion, bit_level):
    return jax.tree.map(
        lambda part, own: part.astype(own.dtype),
        partner(as_sent(portion), "hid", bit_level),
        portion,
    )


def swap_updates(portion, bit_level):
    return jax.tree.map(
        lambda part, own: part.astype(own.dtype),
        partner(as_sent(portion), "hid", bit_level),
        portion,
    )


def make_folder(own_rows, root_low_rows, first_row):
    slab_rows = own_rows.shape[1]

    def absorb(running, portion, offset):
        column_slab = lax.dynamic_slice_in_dim(portion, first_row, slab_rows, 2)
        products = jnp.einsum("brk,bnk->brn", own_rows, portion, preferred_element_type=jnp.float32)
        right_rows = jnp.einsum(
            "bnr,bnk->brk", column_slab, portion, preferred_element_type=jnp.float32
        )
        left_applied = jnp.einsum(
            "brn,bnk->brk", root_low_rows, portion, preferred_element_type=jnp.float32
        )
        return (products, right_rows, left_applied)

    return absorb


def on_device(activations, cotangent, left_gram, right_gram, left_root, right_root):
    owned_blocks, slab_rows, block_size = left_gram.shape
    slab_width = cotangent.shape[1]
    group_size = block_size // slab_width
    block_rows = activations.shape[1] // block_size
    partial_value = jnp.einsum(
        "td,tc->dc", activations, cotangent, preferred_element_type=jnp.float32
    )
    partial_value = partial_value.reshape(block_rows, block_size, slab_width)
    first_row = lax.axis_index("tok") * slab_rows
    left_low = left_root.astype(jnp.bfloat16)
    right_low = right_root.astype(jnp.bfloat16)
    left_full, right_full = (
        lax.all_gather(left_low, "tok", axis=1, tiled=True),
        lax.all_gather(right_low, "tok", axis=1, tiled=True),
    )
    empty = jnp.zeros((owned_blocks, slab_rows, block_size), jnp.float32)
    initial = (empty, empty, empty)
    summed = lax.psum(partial_value.astype(jnp.bfloat16), "tok")
    pieces = summed.reshape(group_size, owned_blocks, block_size, slab_width)
    arrived = butterfly(pieces, swap_blocks)
    full_block = arrived.transpose(1, 2, 0, 3).reshape(owned_blocks, block_size, block_size)
    own_rows = lax.dynamic_slice_in_dim(full_block, first_row, slab_rows, 1)
    folder = make_folder(own_rows, left_low, first_row)
    left_cols, right_rows, left_applied = folder(initial, full_block, 0)
    left_next = BETA * left_gram + left_cols
    right_next = BETA * right_gram + right_rows
    left_refined = newton_rows(left_next, left_full, left_root)
    right_refined = newton_rows(right_next, right_full, right_root)
    precond = jnp.einsum(
        "brk,bkc->brc",
        left_applied.astype(jnp.bfloat16),
        right_full,
        preferred_element_type=jnp.float32,
    )
    squares = lax.psum(jnp.sum(precond * precond, axis=(1, 2)), "tok")
    scale = jnp.sqrt(squares / (block_size * block_size) + EPS)
    scaled = precond / scale[:, None, None]
    outgoing = scaled.reshape(owned_blocks, slab_rows, group_size, slab_width).transpose(2, 0, 1, 3)
    returned = butterfly(outgoing, swap_updates)
    update = returned.reshape(block_rows, slab_rows, slab_width)
    return (left_next, right_next, left_refined, right_refined, update)


RIGHT_PARTS = (4,)
LEFT_PARTS = (2, 2)
VMEM = 60 * 1024 * 1024


def part_ranges(sizes, blocks):
    if sum(sizes) != blocks:
        sizes = (blocks,)
    ranges, first = [], 0
    for size in sizes:
        ranges.append((first, size))
        first += size
    return ranges


def pair_swap(value, axis, mask):
    count = lax.axis_size(axis)
    return lax.ppermute(value, axis, [(i, i ^ mask) for i in range(count)])


def strip_rows(blocks):
    return -(-blocks // 16) * 16


def diagonal_masks(half):
    row = lax.broadcasted_iota(jnp.int32, (half, half), 0)
    column = lax.broadcasted_iota(jnp.int32, (half, half), 1)
    return row, column


def pack_body(ranges, root_ref, fold_ref, *outs):
    total = ranges[-1][0] + ranges[-1][1]
    tile = root_ref.shape[1]
    half = tile // 2
    b = pl.program_id(0)
    me = lax.axis_index("tok")
    low = me < 2

    def tile_at(index):
        return root_ref[0, :, pl.ds(pl.multiple_of(index * tile, tile), tile)]

    own = tile_at(me)
    first, last = own[:half, :half], own[half:, half:]
    row, column = diagonal_masks(half)
    folded = jnp.where(row <= column, first, last)
    place = pl.ds(pl.multiple_of(b * half, half), half)
    fold_ref[place, :half] = folded.astype(jnp.bfloat16)
    fold_ref[place, half:] = own[:half, half:].astype(jnp.bfloat16)
    diagonal = jnp.sum(jnp.where(row == column, last, 0.0), axis=0, keepdims=True)
    strip = strip_rows(total)
    strip_at = pl.ds(total * half, strip)
    line = lax.broadcasted_iota(jnp.int32, (strip, half), 0)

    @pl.when(b == 0)
    def _():
        fold_ref[strip_at, :] = jnp.zeros((strip, tile), jnp.bfloat16)

    held = fold_ref[strip_at, :half].astype(jnp.float32)
    fold_ref[strip_at, :half] = jnp.where(line == b, diagonal, held).astype(jnp.bfloat16)
    near = jnp.where(low, 2, 1)
    far = jnp.where(low, 3, 0)
    mate = jnp.where(me % 2 == 0, me + 1, me - 1)
    outs[-1][pl.ds(pl.multiple_of(b * tile, tile), tile), :] = tile_at(mate).astype(jnp.bfloat16)
    for wide, (start, size) in zip(outs, ranges):

        @pl.when((b >= start) & (b < start + size))
        def _():
            slot = b - start
            wide[pl.ds(pl.multiple_of(slot * 2 * tile, tile), tile), :] = tile_at(near).astype(jnp.bfloat16)
            wide[pl.ds(pl.multiple_of(slot * 2 * tile + tile, tile), tile), :] = tile_at(far).astype(jnp.bfloat16)


def pack(roots, ranges):
    blocks, tile, order = roots.shape
    shapes = [jax.ShapeDtypeStruct((blocks * (tile // 2) + strip_rows(blocks), tile), jnp.bfloat16)]
    for _, size in ranges:
        shapes.append(jax.ShapeDtypeStruct((size * 2 * tile, tile), jnp.bfloat16))
    shapes.append(jax.ShapeDtypeStruct((blocks * tile, tile), jnp.bfloat16))
    return pl.pallas_call(
        functools.partial(pack_body, ranges),
        grid=(blocks,),
        in_specs=[pl.BlockSpec((1, tile, order), lambda b: (b, 0, 0))],
        out_specs=[pl.BlockSpec(one.shape, lambda b: (0, 0)) for one in shapes],
        out_shape=shapes,
        cost_estimate=pl.CostEstimate(
            flops=2 * blocks * tile * order, bytes_accessed=6 * blocks * tile * order, transcendentals=0
        ),
        compiler_params=pltpu.CompilerParams(vmem_limit_bytes=VMEM),
    )(roots)


def join_rows(arrays, pieces):
    total = sum(stop - start for _, start, stop in pieces)
    out = jax.ShapeDtypeStruct((total, arrays[0].shape[1]), arrays[0].dtype)

    def body(*refs):
        at = 0
        for which, start, stop in pieces:
            refs[-1][at : at + stop - start, :] = refs[which][start:stop, :]
            at += stop - start

    return pl.pallas_call(
        body,
        out_shape=out,
        cost_estimate=pl.CostEstimate(flops=total, bytes_accessed=4 * total * out.shape[1], transcendentals=0),
        compiler_params=pltpu.CompilerParams(vmem_limit_bytes=VMEM),
    )(*arrays)


def exchange(roots, ranges):
    fold, *wides, thin = pack(roots, ranges)
    cut = roots.shape[0] * roots.shape[1] // 2
    mate = pair_swap(fold, "tok", 1)
    arrived = []
    for wide in wides:
        arrived.append(pair_swap(wide, "tok", 1))
    rows = fold.shape[0]
    pieces = [(0, 0, thin.shape[0]), (1, 0, cut), (2, 0, cut), (1, cut, rows), (2, cut, rows)]
    joined = join_rows([thin, fold, mate], pieces)
    middle = lax.ppermute(joined, "tok", [(2, 1), (1, 2)])
    outer = lax.ppermute(middle, "tok", [(1, 0), (2, 3)])
    return arrived, (mate, middle, outer)


def front_body(place_ref, act, cots, left_gram, right_gram, left_root, pieces, left_next, right_next, applied, tokens, cot, grad):
    step = pl.program_id(0)
    rows, order = left_gram.shape[1:]
    group, width = act.shape[0], pieces[0].shape[1]
    first_row = place_ref[1] * rows
    odd = place_ref[0] % 2
    tokens[:group, :] = act[...]
    for at, one in enumerate(cots):
        cot[at * group : (at + 1) * group, :] = one[...]
    for at in range(len(pieces) // 2):

        @pl.when(step == at)
        def _():
            tokens[group:, pl.ds(pl.multiple_of(odd * width, width), width)] = pieces[2 * at][...]
            tokens[group:, pl.ds(pl.multiple_of((1 - odd) * width, width), width)] = pieces[2 * at + 1][...]

    both = (((0,), (0,)), ((), ()))

    @pl.loop(0, order // rows)
    def _(part):
        chunk = pl.ds(pl.multiple_of(part * rows, rows), rows)
        grad[chunk, :] = lax.dot_general(
            tokens[:, chunk], cot[...], both, preferred_element_type=jnp.float32
        ).astype(jnp.bfloat16)

    slab = pl.ds(pl.multiple_of(first_row, rows), rows)
    product = lax.dot_general(
        grad[slab, :], grad[...], (((1,), (1,)), ((), ())), preferred_element_type=jnp.float32
    )
    left_next[0] = BETA * left_gram[0] + product
    product = lax.dot_general(grad[:, slab], grad[...], both, preferred_element_type=jnp.float32)
    right_next[0] = BETA * right_gram[0] + product
    applied[0] = jnp.dot(
        left_root[0].astype(jnp.bfloat16), grad[...], preferred_element_type=jnp.float32
    ).astype(jnp.bfloat16)


def front(place, act, cots, pieces, left_gram, right_gram, left_root, first, base):
    blocks, rows, order = left_gram.shape
    count = len(pieces)
    groups = len(cots)
    depth, width = groups * act.shape[0], cots[0].shape[1]
    size = count // 2
    held = 0 if base is None else len(base)

    def body(place_ref, act_ref, lg, rg, lr, *refs):
        cot_refs, refs = refs[:groups], refs[groups:]
        front_body(place_ref, act_ref, cot_refs, lg, rg, lr, refs[:count], *refs[count + held :])

    def whole(array):
        return pl.BlockSpec(array.shape, lambda b, s: (0,) * array.ndim)

    def block_of(b, s):
        return jnp.bitwise_xor(s[0] // 2, b + first)

    slab = pl.BlockSpec((1, rows, order), lambda b, s: (block_of(b, s), 0, 0))
    columns = pl.BlockSpec((act.shape[0], order), lambda b, s: (0, block_of(b, s)))
    shape = (blocks, rows, order)
    operands = [place, act, left_gram, right_gram, left_root, *cots, *pieces]
    specs = [columns, slab, slab, slab] + [whole(one) for one in (*cots, *pieces)]
    aliases = {}
    if base is not None:
        aliases = {len(operands) + k: k for k in range(held)}
        operands += base
        specs += [pl.BlockSpec(memory_space=pl.ANY)] * held
    return pl.pallas_call(
        body,
        grid_spec=pltpu.PrefetchScalarGridSpec(
            num_scalar_prefetch=1,
            grid=(size,),
            in_specs=specs,
            out_specs=[slab, slab, slab],
            scratch_shapes=[
                pltpu.VMEM((depth, order), jnp.bfloat16),
                pltpu.VMEM((depth, width), jnp.bfloat16),
                pltpu.VMEM((order, order), jnp.bfloat16),
            ],
        ),
        out_shape=[
            jax.ShapeDtypeStruct(shape, jnp.float32),
            jax.ShapeDtypeStruct(shape, jnp.float32),
            jax.ShapeDtypeStruct(shape, jnp.bfloat16),
        ],
        input_output_aliases=aliases,
        cost_estimate=pl.CostEstimate(
            flops=2 * size * order * order * (depth + 3 * rows),
            bytes_accessed=size * rows * order * 22,
            transcendentals=0,
        ),
        compiler_params=pltpu.CompilerParams(vmem_limit_bytes=VMEM),
    )(*operands)


def chain_body(first, total, with_update, with_base, with_scale, *refs):
    next_ref, root_ref, wide, middle, outer, fold, strip_ref = refs[:7]
    far_refs, refs = refs[7:15], refs[15:]
    if with_update:
        applied, refs = refs[0], refs[1:]
    if with_scale:
        scale_ref, unscaled, refs = refs[0], refs[1], refs[2:]
    if with_base:
        refs = refs[1:]
    refined, refs = refs[0], refs[1:]
    if with_scale:
        scaled, refs = refs[0], refs[1:]
        many = unscaled.shape[0]
        for at in range(many):
            scaled[at] = unscaled[at] * scale_ref[pl.program_id(0) * many + at]
    if with_update:
        precond, energy, refs = refs[0], refs[1], refs[2:]
    full, product = refs
    tile = root_ref.shape[1]
    half = tile // 2
    b = pl.program_id(0) + first
    me = lax.axis_index("tok")
    low = me < 2
    end = (me == 0) | (me == 3)
    near = jnp.where(low, 2, 1)
    far = jnp.where(low, 3, 0)
    mate = jnp.where(me % 2 == 0, me + 1, me - 1)

    def at(index, extra=0, size=tile):
        return pl.ds(pl.multiple_of(index * tile + extra, half), size)

    def flipped(value):
        return value.astype(jnp.float32).T.astype(jnp.bfloat16)

    full[at(me), :] = root_ref[0].astype(jnp.bfloat16)
    for other in (mate, near, far):
        full[at(other), at(me)] = root_ref[0, :, at(other)].T.astype(jnp.bfloat16)
    row, column = diagonal_masks(half)
    strip = strip_rows(total)
    line = lax.broadcasted_iota(jnp.int32, (strip, half), 0)

    def unfold(index, folded, corner, held):
        folded, held = folded.astype(jnp.float32), held.astype(jnp.float32)
        turned = folded.T
        diagonal = jnp.sum(jnp.where(line == b, held, 0.0), axis=0, keepdims=True)
        full[at(index, 0, half), at(index, 0, half)] = jnp.where(row <= column, folded, turned).astype(jnp.bfloat16)
        lower = jnp.where(row == column, diagonal, jnp.where(row > column, folded, turned))
        full[at(index, half, half), at(index, half, half)] = lower.astype(jnp.bfloat16)
        full[at(index, 0, half), at(index, half, half)] = corner
        full[at(index, half, half), at(index, 0, half)] = flipped(corner)

    def both(i, j, value):
        full[at(i), at(j)] = value
        full[at(j), at(i)] = flipped(value)

    def arrived(k, columns):
        return jnp.where(end, far_refs[k + 4][:, columns], far_refs[k][:, columns])

    left, right = slice(0, half), slice(half, tile)
    unfold(mate, fold[:, left], fold[:, right], strip_ref[:, left])
    unfold(near, arrived(0, left), arrived(0, right), arrived(1, left))
    unfold(far, arrived(2, left), arrived(2, right), arrived(3, left))
    both(mate, near, wide[:tile, :])
    both(mate, far, wide[tile:, :])
    both(near, far, jnp.where(end, outer[...], middle[...]))
    if with_update:
        value = jnp.dot(applied[0], full[...], preferred_element_type=jnp.float32)
        precond[0] = value
        energy[0] = jnp.sum((value * value).reshape(-1, 8, value.shape[1]), axis=0)
    product[...] = next_ref[0].astype(jnp.bfloat16)

    for _ in range(4):
        product[...] = jnp.dot(
            product[...], full[...], preferred_element_type=jnp.float32
        ).astype(jnp.bfloat16)

    final = jnp.dot(product[...], full[...], preferred_element_type=jnp.float32)
    refined[0] = (5.0 * root_ref[0] - final) / 4.0


def chain(next_rows, roots, wide, messages, applied, base, first, size, scaling=None):
    blocks, rows, order = roots.shape

    def slab(array):
        return pl.BlockSpec((1,) + array.shape[1:], lambda b: (b + first, 0, 0))

    half, strip = rows // 2, strip_rows(blocks)

    def fold_specs(offset, slots):
        def folded(slot):
            start = (offset + slot * blocks * half) // half
            return pl.BlockSpec((half, rows), lambda b: (b + first + start, 0))

        def diagonal(slot):
            start = (offset + slots * blocks * half) // strip + slot
            return pl.BlockSpec((strip, rows), lambda b: (start, 0))

        return [spec for slot in range(slots) for spec in (folded(slot), diagonal(slot))]

    fold, middle, outer = messages
    offset = blocks * rows
    operands = [next_rows, roots, wide, middle, outer, fold, fold] + [middle] * 4 + [outer] * 4
    specs = [slab(next_rows), slab(roots), pl.BlockSpec((2 * rows, rows), lambda b: (b, 0))]
    specs += [pl.BlockSpec((rows, rows), lambda b: (b + first, 0))] * 2
    specs += fold_specs(0, 1) + fold_specs(offset, 2) * 2
    if applied is not None:
        operands.append(applied)
        specs.append(slab(applied))
    aliases = {}
    if scaling is not None:
        operands += scaling
        share = pl.BlockSpec((blocks // size, rows, order), lambda b: (b, 0, 0))
        specs += [pl.BlockSpec(memory_space=pltpu.SMEM), share]
    if base is not None:
        aliases = {len(operands): 0}
        operands.append(base)
        specs.append(pl.BlockSpec(memory_space=pl.ANY))
    out = jax.ShapeDtypeStruct((blocks, rows, order), jnp.float32)
    outputs = [out] if applied is None else [out, out, jax.ShapeDtypeStruct((blocks, 8, order), jnp.float32)]
    out_specs = [slab(one) for one in outputs]
    if scaling is not None:
        outputs.append(out)
        out_specs.append(share)
    matmuls = 5 if applied is None else 6
    return pl.pallas_call(
        functools.partial(
            chain_body, first, blocks, applied is not None, base is not None, scaling is not None
        ),
        grid=(size,),
        in_specs=specs,
        out_specs=out_specs,
        out_shape=outputs,
        input_output_aliases=aliases,
        scratch_shapes=[
            pltpu.VMEM((order, order), jnp.bfloat16),
            pltpu.VMEM((rows, order), jnp.bfloat16),
        ],
        cost_estimate=pl.CostEstimate(
            flops=2 * matmuls * size * rows * order * order,
            bytes_accessed=size * rows * order * 20,
            transcendentals=0,
        ),
        compiler_params=pltpu.CompilerParams(vmem_limit_bytes=VMEM),
    )(*operands)


def gather_tokens(activations, cotangent):
    count = lax.axis_size("hid")
    place = lax.axis_index("hid")
    width = activations.shape[1] // count
    piece = lax.dynamic_slice_in_dim(activations, place * width, width, 1)
    arrived, cots = [], [cotangent]
    for mask in (1, 2, 3):
        arrived.append(pair_swap(piece, "tok", mask))
    for mask in (1, 2, 3):
        cots.append(pair_swap(cotangent, "tok", mask))
    mine = join_rows(arrived, [(at, 0, one.shape[0]) for at, one in enumerate(arrived)])
    held = [mine]
    for mask in range(2, count, 2):
        held.append(pair_swap(mine, "hid", mask))
    pieces = []
    for one in held:
        pieces += [one, pair_swap(one, "hid", 1)]
    return pieces, cots


def line_program(activations, cotangent, left_gram, right_gram, left_root, right_root):
    blocks, _, order = left_gram.shape
    right_ranges = part_ranges(RIGHT_PARTS, blocks)
    left_ranges = part_ranges(LEFT_PARTS, blocks)
    pieces, cots = gather_tokens(activations, cotangent)
    right_wide, right_messages = exchange(right_root, right_ranges)
    left_wide, left_messages = exchange(left_root, left_ranges)
    place = jnp.stack([lax.axis_index("hid"), lax.axis_index("tok")]).astype(jnp.int32)
    base = None
    share = max(2, len(pieces) // 2)
    for at in range(0, len(pieces), share):
        base = front(
            place, activations, cots, pieces[at : at + share],
            left_gram, right_gram, left_root, at // 2, base,
        )
    left_next, right_next, applied = base
    (first, size), = right_ranges
    right_refined, precond, energy = chain(
        right_next, right_root, right_wide[0], right_messages, applied, None, first, size
    )
    local = jnp.sum(energy, axis=(1, 2))
    squares = local
    for mask in (1, 2, 3):
        squares = squares + pair_swap(local, "tok", mask)
    scale = 1.0 / jnp.sqrt(squares / (order * order) + EPS)
    left_refined = update = None
    for at, (first, size) in enumerate(left_ranges):
        last = at == len(left_ranges) - 1 and blocks % size == 0
        left_refined, *update = chain(
            left_next, left_root, left_wide[at], left_messages, None, left_refined,
            first, size, [scale, precond] if last else None
        )
    update = update[0] if update else precond * scale[:, None, None]
    return left_next, right_next, left_refined, right_refined, update


def solution(mesh):
    in_specs = (
        P("tok", None),
        P("tok", "hid"),
        P("hid", "tok", None),
        P("hid", "tok", None),
        P("hid", "tok", None),
        P("hid", "tok", None),
    )
    out_specs = (
        P("hid", "tok", None),
        P("hid", "tok", None),
        P("hid", "tok", None),
        P("hid", "tok", None),
        P(None, "tok", "hid"),
    )

    def run(*operands):
        activations, cotangent, left_gram = (one.shape for one in operands[:3])
        tok, hid = mesh.shape["tok"], mesh.shape["hid"]
        whole_blocks = cotangent[1] == left_gram[2]
        one_column = left_gram[0] == activations[1] // left_gram[2]
        even = hid >= 4 and hid & (hid - 1) == 0
        halves = 2 * left_gram[0] == hid
        if tok == 4 and whole_blocks and one_column and even and halves:
            return line_program(*operands)
        return on_device(*operands)

    return jax.shard_map(
        run, mesh=mesh, in_specs=in_specs, out_specs=out_specs, check_vma=False
    )
```
